256 devices in a mesh: ta: 2 (over x_hi), gx: 128 (over x_lo, z, y, core).
Axes of the slice: x: 4 (x_hi: 2, x_lo: 2; x = x_hi * 2 + x_lo), y: 4, z: 8, core: 2. Of those that a mesh axis runs over, the one named last changes fastest.
Arguments:
- voltages: bfloat16 [2, 128, 2, 256, 512], P('ta', 'gx'), may hold values from -6 to 6
- weights: bfloat16 [2, 256, 2, 512, 64], P(None, 'gx'), may hold values from -0.125 to 0.125
Outputs:
- spectra: float32 [256, 2, 512, 64], P(None, None, 'gx', 'ta')
The draws below stay inside these ranges and needn't reach their ends.
All inputs are finite; a program needn't handle non-finite values.
Results may differ from the reference program's by a relative error of at most 0.0003.
Values may be sent and summed in bfloat16 or wider, within the bound.
A program may use at most 64 MiB of HBM per device.

```python
import jax
import jax.numpy as jnp
from jax import lax

ANTENNA_COUNT = 64
BEAM_TOTAL = 512
CHANNEL_COUNT = 512
HALF_SAMPLES = 512


def block_levels(own_key, shape, cuts, low, largest):
    factor_of = 1.0
    for position, blocks in cuts:
        draws = jax.random.uniform(jax.random.fold_in(jax.random.fold_in(own_key, 6), position), (blocks,), jnp.float32, low / len(cuts), largest / len(cuts))
        factor_of = factor_of * jnp.repeat(jnp.exp(draws), shape[position] // blocks).reshape((-1,) + (1,) * (len(shape) - 1 - position))
    return factor_of


def normal_values(rng, dims, scale, most, pieces=(), dtype=jnp.bfloat16):
    array = scale * jax.random.normal(rng, dims, jnp.float32)
    if pieces:
        array = array * block_levels(rng, dims, pieces, -0.22, 0.18)
    return jnp.clip(array, -most, most).astype(dtype)


def setup_inputs(seed: int = 0) -> dict:
    streams_of = jax.random.split(jax.random.key(seed), 3)
    voltages = normal_values(streams_of[0], (2, 2 * ANTENNA_COUNT, 2, CHANNEL_COUNT // 2, HALF_SAMPLES), 1.0, 6.0, ((0, 2), (1, 128)))
    weights = normal_values(streams_of[1], (2, CHANNEL_COUNT // 2, 2, BEAM_TOTAL, ANTENNA_COUNT), (32 * ANTENNA_COUNT) ** -0.5, 0.125, ((1, 128),))
    return dict(voltages=voltages, weights=weights)


def beam_power(voltage, weight_block):
    antennas = weight_block.shape[3]
    beam_count = weight_block.shape[2]
    powers = []
    for side_index in range(2):
        real_w = weight_block[side_index, 0]
        imag_w = weight_block[side_index, 1]
        upper_rows = jnp.stack([real_w, -imag_w], axis=-1).reshape(beam_count, 2 * antennas)
        bottom_half_rows = jnp.stack([imag_w, real_w], axis=-1).reshape(beam_count, 2 * antennas)
        matrix = jnp.concatenate([upper_rows, bottom_half_rows], 0)
        signal = voltage[side_index * antennas:(side_index + 1) * antennas].reshape(2 * antennas, -1)
        beam_voltage_field = jnp.dot(matrix, signal, preferred_element_type=jnp.float32)
        power = beam_voltage_field[:beam_count] * beam_voltage_field[:beam_count] + beam_voltage_field[beam_count:] * beam_voltage_field[beam_count:]
        powers.append(power.reshape(beam_count, -1, 8).sum(-1))
    return jnp.stack(powers, 0)


def reference(voltages, weights):
    moved = jnp.moveaxis(voltages, 3, 0)
    weight_moved = jnp.moveaxis(weights, 1, 0)

    def one_channel(paired):
        voltage, weight_block = paired
        return beam_power(voltage[0], weight_block) + beam_power(voltage[1], weight_block)

    return lax.map(one_channel, (moved, weight_moved))
```

```python
import jax
import jax.numpy as jnp
from jax import lax
from jax.experimental import pallas as pl
from jax.experimental.pallas import tpu as pltpu
from jax.sharding import PartitionSpec as P

MESH = pl.DeviceIdType.MESH
BF = jnp.bfloat16
F32 = jnp.float32
NX, NY, NZ, NC = 4, 4, 8, 2
FAR_Z = (4, 3, 5, 2, 6, 1, 7, 0)


def iota(shape, dim):
    return lax.broadcasted_iota(jnp.int32, shape, dim)


def one_hot(cond):
    return jnp.where(cond, 1.0, 0.0).astype(BF)


def dot(a, b):
    return jnp.dot(a, b, preferred_element_type=F32)


def tn_dot(a, b):
    return lax.dot_general(a, b, (((0,), (0,)), ((), ())), preferred_element_type=F32)


def place():
    ta = lax.axis_index("ta")
    g = lax.axis_index("gx")
    core = lax.rem(g, 2)
    y = lax.rem(lax.div(g, 2), NY)
    z = lax.rem(lax.div(g, 8), NZ)
    x = ta * 2 + lax.div(g, 64)
    return ta, g, x, y, z, core


def exchange_kernel(x_hbm, w_hbm, out_ref, xv, wv, snd, rcv, amat, acc, snd2, rcv2,
                    in_sem, send_sem, recv_sem, send2_sem, recv2_sem):
    ta, g, x, y, z, core = place()
    me = ta * 128 + g
    copy_x = pltpu.make_async_copy(x_hbm, xv, in_sem.at[0])
    copy_w = pltpu.make_async_copy(w_hbm, wv, in_sem.at[1])
    copy_x.start()
    copy_w.start()

    zs = [lax.rem(z + d, NZ) * 8 for d in range(NZ)]
    cores = [core, 1 - core]

    def xy_of(i):
        dx = lax.rem(lax.div(i, 4) + 2, NX)
        dy = lax.rem(i + 2, NY)
        nx = lax.rem(x + dx, NX)
        ny = lax.rem(y + dy, NY)
        return lax.div(nx, 2), lax.rem(nx, 2) * 64 + ny * 2

    def targets(i, skip_self):
        nta, base = xy_of(i)
        for dz in FAR_Z:
            for dc in range(NC):
                if skip_self and dz == 0 and dc == 0:
                    continue
                yield nta, base + zs[dz] + cores[dc]

    barrier = pltpu.get_barrier_semaphore()

    def greet(nta, ng):
        pl.semaphore_signal(barrier, inc=1, device_id={"ta": nta, "gx": ng}, device_id_type=MESH)

    def greet_step(i, carry):
        for nta, ng in targets(i, False):
            greet(nta, ng)
        return carry

    lax.fori_loop(0, 10, greet_step, 0)
    lax.fori_loop(11, 16, greet_step, 0)
    for nta, ng in targets(10, True):
        greet(nta, ng)

    copy_x.wait()
    r_i, r_k = iota((128, 128), 0), iota((128, 128), 1)
    rows = one_hot(r_k == ((r_i >> 1) & 1) * 64 + (r_i >> 2) * 2 + (r_i & 1))
    p_i, p_k = iota((256, 256), 0), iota((256, 256), 1)
    lanes = one_hot(p_i == (p_k & 31) * 8 + (p_k >> 5))
    snd_rows = snd.reshape(1024, 256)
    for blk in range(4):
        block = jnp.concatenate([xv[0, blk * 64:(blk + 1) * 64], xv[1, blk * 64:(blk + 1) * 64]], 0)
        grouped = dot(rows, block).astype(BF)
        for h in range(2):
            piece = dot(grouped[:, h * 256:(h + 1) * 256], lanes).astype(BF)
            snd_rows[pl.ds(h * 512 + blk * 128, 128), :] = piece

    pl.semaphore_wait(barrier, 255)

    def send(nta, ng):
        pltpu.make_async_remote_copy(
            snd.at[nta * 128 + ng], rcv.at[me], send_sem, recv_sem,
            device_id={"ta": nta, "gx": ng}, device_id_type=MESH).start()

    def send_step(i, carry):
        for nta, ng in targets(i, False):
            send(nta, ng)
        return carry

    lax.fori_loop(0, 10, send_step, 0)
    lax.fori_loop(11, 16, send_step, 0)
    for nta, ng in targets(10, True):
        send(nta, ng)
    rcv[me] = snd[me]

    copy_w.wait()
    e_i, e_k = iota((128, 512), 0), iota((128, 512), 1)
    e_ri, e_a = e_i >> 6, e_i & 63
    k_c, k_a, k_ri, k_j = e_k >> 8, (e_k >> 2) & 63, (e_k >> 1) & 1, e_k & 1
    same = e_a == k_a
    sign = jnp.where((k_c == 0) & (k_ri == 1), -1.0, 1.0)
    for j in range(2):
        spread = jnp.where(same & (e_ri == (k_c ^ k_ri)) & (k_j == j), sign, 0.0).astype(BF)
        for q in range(2):
            both = wv[q, j].reshape(128, 512)
            made = tn_dot(both, spread).astype(BF)
            amat[j * 2 + q, 0:512, :] = made[:, 0:256]
            amat[j * 2 + q, 512:1024, :] = made[:, 256:512]

    pltpu.make_async_copy(snd.at[pl.ds(0, 255)], rcv.at[pl.ds(0, 255)], recv_sem).wait()

    rcv_rows = rcv.reshape(1024, 256)

    def channel(i, carry):
        q = lax.rem(i, 2)
        total = None
        for h in range(2):
            signal = rcv_rows[pl.ds(pl.multiple_of(h * 512 + q * 256, 256), 256), :]
            field = dot(amat[i], signal)
            re, im = field[0:512], field[512:1024]
            power = re * re + im * im
            part = power[:, 0:128] + power[:, 128:256]
            total = part if total is None else total + part
        acc[i] = total
        return carry

    lax.fori_loop(0, 4, channel, 0)

    lane = iota((512, 128), 1)
    low, even = lane < 64, (lane & 32) == 0
    fold = []
    for i in range(2):
        a, b = acc[i], acc[i + 2]
        fold.append(jnp.where(low, a, b) + pltpu.roll(jnp.where(low, b, a), 64, 1))
    other = jnp.where(even, fold[1], fold[0])
    summed = jnp.where(even, fold[0], fold[1]) + jnp.where(
        even, pltpu.roll(other, 96, 1), pltpu.roll(other, 32, 1))
    snd2.reshape(512, 128)[...] = summed

    def send2(ng):
        pltpu.make_async_remote_copy(
            snd2.at[ng], rcv2.at[g], send2_sem, recv2_sem,
            device_id={"ta": ta, "gx": ng}, device_id_type=MESH).start()

    x_lo = lax.div(g, 64)

    def send2_step(i, carry):
        base = lax.rem(x_lo + lax.div(i, 4), 2) * 64 + lax.rem(y + i + 1, NY) * 2
        for dz in FAR_Z:
            for dc in range(NC):
                send2(base + zs[dz] + cores[dc])
        return carry

    lax.fori_loop(0, 3, send2_step, 0)
    lax.fori_loop(4, 8, send2_step, 0)
    base = x_lo * 64 + y * 2
    for dz in FAR_Z:
        for dc in range(NC):
            if dz or dc:
                send2(base + zs[dz] + cores[dc])
    rcv2[g] = snd2[g]
    pltpu.make_async_copy(snd2.at[pl.ds(0, 127)], rcv2.at[pl.ds(0, 127)], recv2_sem).wait()
    out_ref[...] = rcv2[...]
    pltpu.make_async_copy(snd.at[pl.ds(0, 255)], rcv.at[pl.ds(0, 255)], send_sem).wait()
    pltpu.make_async_copy(snd2.at[pl.ds(0, 127)], rcv2.at[pl.ds(0, 127)], send2_sem).wait()


def layout_kernel(r_ref, out_ref):
    lane = iota((32, 128), 1)
    half = lane >> 1
    odd = (lane & 1) == 1
    for b in range(4):
        turned = r_ref[:, b, :].T
        for q in range(2):
            first = turned[q * 32:(q + 1) * 32]
            second = turned[64 + q * 32:64 + (q + 1) * 32]
            for part in range(2):
                index = half + part * 64
                out_ref[q, b, :, part * 128:(part + 1) * 128] = jnp.where(
                    odd, jnp.take_along_axis(second, index, axis=1),
                    jnp.take_along_axis(first, index, axis=1))


def solution(mesh):
    def on_device(voltages, weights):
        vmem = pl.BlockSpec(memory_space=pltpu.VMEM)
        hbm = pl.BlockSpec(memory_space=pl.ANY)
        got = pl.pallas_call(
            exchange_kernel,
            out_shape=jax.ShapeDtypeStruct((128, 4, 128), F32),
            in_specs=[hbm, hbm],
            out_specs=vmem,
            scratch_shapes=[
                pltpu.VMEM((2, 256, 512), BF),
                pltpu.VMEM((2, 2, 2, 64, 512), BF),
                pltpu.VMEM((256, 4, 256), BF),
                pltpu.VMEM((256, 4, 256), BF),
                pltpu.VMEM((4, 1024, 256), BF),
                pltpu.VMEM((4, 512, 128), F32),
                pltpu.VMEM((128, 4, 128), F32),
                pltpu.VMEM((128, 4, 128), F32),
                pltpu.SemaphoreType.DMA((2,)),
                pltpu.SemaphoreType.DMA,
                pltpu.SemaphoreType.DMA,
                pltpu.SemaphoreType.DMA,
                pltpu.SemaphoreType.DMA,
            ],
            compiler_params=pltpu.CompilerParams(collective_id=0, has_side_effects=True),
        )(voltages[0, 0], jnp.swapaxes(weights, 3, 4))
        out = pl.pallas_call(
            layout_kernel,
            out_shape=jax.ShapeDtypeStruct((2, 4, 32, 256), F32),
            in_specs=[vmem],
            out_specs=vmem,
        )(got)
        return jnp.transpose(out, (3, 0, 1, 2))

    return jax.shard_map(
        on_device,
        mesh=mesh,
        in_specs=(P("ta", "gx", None, None, None), P(None, "gx", None, None, None)),
        out_specs=P(None, None, "gx", "ta"),
        check_vma=False,
    )
```

```python
import jax
import jax.numpy as jnp
from jax import lax
from jax.experimental import pallas as pl
from jax.experimental.pallas import tpu as pltpu
from jax.sharding import PartitionSpec as P

MESH = pl.DeviceIdType.MESH
BF = jnp.bfloat16
F32 = jnp.float32
NX, NY, NZ, NC = 4, 4, 8, 2


def iota(shape, dim):
    return lax.broadcasted_iota(jnp.int32, shape, dim)


def one_hot(cond):
    return jnp.where(cond, 1.0, 0.0).astype(BF)


def dot(a, b):
    return jnp.dot(a, b, preferred_element_type=F32)


def tn_dot(a, b):
    return lax.dot_general(a, b, (((0,), (0,)), ((), ())), preferred_element_type=F32)


def exchange_kernel(x_hbm, w_hbm, out_ref, xv, wv, snd, rcv, amat, acc, snd2, rcv2,
                    plane_sem, in_sem, send_sem, recv_sem, send2_sem, recv2_sem):
    ta = lax.axis_index("ta")
    g = lax.axis_index("gx")
    core = lax.rem(g, 2)
    y = lax.rem(lax.div(g, 2), NY)
    z = lax.rem(lax.div(g, 8), NZ)
    x_lo = lax.div(g, 64)
    x = ta * 2 + x_lo
    me = ta * 128 + g
    copy_x = pltpu.make_async_copy(x_hbm, xv, in_sem.at[0])
    copy_w = pltpu.make_async_copy(w_hbm, wv, in_sem.at[1])
    copy_x.start()
    copy_w.start()

    nxs = [lax.rem(x + d, NX) for d in range(NX)]
    tas = [lax.div(v, 2) for v in nxs]
    xbs = [lax.rem(v, 2) * 64 for v in nxs]
    ybs = [lax.rem(y + d, NY) * 2 for d in range(NY)]
    cores = [core, 1 - core]
    plane = [(tas[dx], xbs[dx] + ybs[dy] + cores[dc])
             for dx in (2, 1, 3, 0) for dy in (2, 1, 3, 0) for dc in (1, 0)]

    def signal(sem, nta, ng):
        pl.semaphore_signal(sem, inc=1, device_id={"ta": nta, "gx": ng}, device_id_type=MESH)

    barrier = pltpu.get_barrier_semaphore()
    line = x_lo * 64 + y * 2 + core
    for nta, base in plane[:-1]:
        signal(barrier, nta, base + z * 8)
    for dz in (4, 3, 5, 2, 6, 1, 7):
        signal(barrier, ta, line + lax.rem(z + dz, NZ) * 8)

    copy_x.wait()
    r_i, r_k = iota((128, 128), 0), iota((128, 128), 1)
    rows = one_hot(r_k == (r_i & 1) * 64 + ((r_i >> 1) & 31) * 2 + (r_i >> 6))
    p_i, p_k = iota((256, 256), 0), iota((256, 256), 1)
    lanes = one_hot(p_i == (p_k & 31) * 8 + (p_k >> 5))
    snd_rows = snd.reshape(1024, 256)
    for blk in range(4):
        block = jnp.concatenate([xv[0, blk * 64:(blk + 1) * 64], xv[1, blk * 64:(blk + 1) * 64]], 0)
        grouped = dot(rows, block).astype(BF)
        for h in range(2):
            piece = dot(grouped[:, h * 256:(h + 1) * 256], lanes).astype(BF)
            for j in range(2):
                snd_rows[pl.ds(j * 512 + h * 256 + blk * 64, 64), :] = piece[j * 64:(j + 1) * 64]

    pl.semaphore_wait(barrier, 38)
    for dz in (4, 3, 5, 2, 6, 1, 7):
        signal(plane_sem.at[z], ta, line + lax.rem(z + dz, NZ) * 8)

    def send(j, nta, ng):
        pltpu.make_async_remote_copy(
            snd.at[j * 256 + nta * 128 + ng], rcv.at[j * 256 + me], send_sem.at[j], recv_sem.at[j],
            device_id={"ta": nta, "gx": ng}, device_id_type=MESH).start()

    def send_plane(j, zz):
        for nta, base in plane:
            send(j, nta, base + zz * 8)

    def send_own(j):
        for nta, base in plane[:-1]:
            send(j, nta, base + z * 8)
        rcv[j * 256 + me] = snd[j * 256 + me]

    group = lax.div(z, 4)

    def other_group(i):
        return (1 - group) * 4 + lax.rem(z + i, 4)

    def own_group(i):
        return group * 4 + lax.rem(z + i, 4)

    def wait_and_send(plane_of, j):
        def step(i, carry):
            zz = plane_of(i)
            pl.semaphore_wait(plane_sem.at[zz], 1)
            send_plane(j, zz)
            return carry
        return step

    def just_send(plane_of, j):
        def step(i, carry):
            send_plane(j, plane_of(i))
            return carry
        return step

    lax.fori_loop(1, 4, wait_and_send(own_group, 0), 0)
    send_own(0)
    lax.fori_loop(0, 4, wait_and_send(other_group, 0), 0)
    lax.fori_loop(0, 4, just_send(other_group, 1), 0)
    lax.fori_loop(1, 4, just_send(own_group, 1), 0)
    send_own(1)

    copy_w.wait()
    b_i, b_k = iota((512, 512), 0), iota((512, 512), 1)
    beams = one_hot(b_i == (b_k & 255) * 2 + (b_k >> 8))
    e_i, e_k = iota((128, 256), 0), iota((128, 256), 1)
    e_ri, e_a = e_i >> 6, e_i & 63
    k_c, k_a, k_ri = e_k >> 7, (e_k >> 1) & 63, e_k & 1
    sign = jnp.where((k_c == 0) & (k_ri == 1), -1.0, 1.0)
    spread = jnp.where((e_a == k_a) & (e_ri == (k_c ^ k_ri)), sign, 0.0).astype(BF)
    for j in range(2):
        for q in range(2):
            both = dot(wv[q, j].reshape(128, 512), beams).astype(BF)
            made = tn_dot(both, spread).astype(BF)
            amat[j * 2 + q, 0:512, :] = made[:, 0:128]
            amat[j * 2 + q, 512:1024, :] = made[:, 128:256]

    rcv_rows = rcv.reshape(1024, 256)
    lane = iota((256, 128), 1)
    low, even = lane < 64, (lane & 32) == 0

    def send2(j, ng):
        pltpu.make_async_remote_copy(
            snd2.at[j * 128 + ng], rcv2.at[j * 128 + g], send2_sem.at[j], recv2_sem.at[j],
            device_id={"ta": ta, "gx": ng}, device_id_type=MESH).start()

    half_plane = [lax.rem(x_lo + dx, 2) * 64 + ybs[dy] + cores[dc]
                  for dx in (1, 0) for dy in (2, 1, 3, 0) for dc in (1, 0)]

    for j in range(2):
        pltpu.make_async_copy(snd.at[pl.ds(0, 255)], rcv.at[pl.ds(0, 255)], recv_sem.at[j]).wait()

        def channel(q, carry):
            total = None
            for h in range(2):
                start = pl.multiple_of(j * 512 + h * 256 + q * 128, 128)
                field = dot(amat[j * 2 + q], rcv_rows[pl.ds(start, 128), :])
                re, im = field[0:512], field[512:1024]
                power = re * re + im * im
                part = power[:, 0:128] + power[:, 128:256]
                total = part if total is None else total + part
            acc[q] = total
            return carry

        lax.fori_loop(0, 2, channel, 0)
        fold = []
        for q in range(2):
            a, b = acc[q, 0:256], acc[q, 256:512]
            fold.append(jnp.where(low, a, b) + pltpu.roll(jnp.where(low, b, a), 64, 1))
        other = jnp.where(even, fold[1], fold[0])
        summed = jnp.where(even, fold[0], fold[1]) + jnp.where(
            even, pltpu.roll(other, 96, 1), pltpu.roll(other, 32, 1))
        snd2.reshape(512, 128)[j * 256:(j + 1) * 256, :] = summed

        def send2_step(i, carry):
            zz = lax.rem(z + i, NZ)
            for base in half_plane:
                send2(j, base + zz * 8)
            return carry

        lax.fori_loop(1, NZ, send2_step, 0)
        for base in half_plane[:-1]:
            send2(j, base + z * 8)
        rcv2[j * 128 + g] = snd2[j * 128 + g]

    for j in range(2):
        pltpu.make_async_copy(snd2.at[pl.ds(0, 127)], rcv2.at[pl.ds(0, 127)], recv2_sem.at[j]).wait()
    out_ref[...] = rcv2[...]
    for j in range(2):
        pltpu.make_async_copy(snd.at[pl.ds(0, 255)], rcv.at[pl.ds(0, 255)], send_sem.at[j]).wait()
        pltpu.make_async_copy(snd2.at[pl.ds(0, 127)], rcv2.at[pl.ds(0, 127)], send2_sem.at[j]).wait()


def layout_kernel(r_ref, out_ref):
    lane = iota((32, 128), 1)
    half = lane >> 1
    odd = (lane & 1) == 1
    for high in range(2):
        turned = [r_ref[j * 128:(j + 1) * 128, high, :].T for j in range(2)]
        for parity in range(2):
            for q in range(2):
                at = parity * 64 + q * 32
                for part in range(2):
                    index = half + part * 64
                    out_ref[q, high * 2 + parity, :, part * 128:(part + 1) * 128] = jnp.where(
                        odd, jnp.take_along_axis(turned[1][at:at + 32], index, axis=1),
                        jnp.take_along_axis(turned[0][at:at + 32], index, axis=1))


def solution(mesh):
    def on_device(voltages, weights):
        vmem = pl.BlockSpec(memory_space=pltpu.VMEM)
        hbm = pl.BlockSpec(memory_space=pl.ANY)
        got = pl.pallas_call(
            exchange_kernel,
            out_shape=jax.ShapeDtypeStruct((256, 2, 128), F32),
            in_specs=[hbm, hbm],
            out_specs=vmem,
            scratch_shapes=[
                pltpu.VMEM((2, 256, 512), BF),
                pltpu.VMEM((2, 2, 2, 64, 512), BF),
                pltpu.VMEM((512, 2, 256), BF),
                pltpu.VMEM((512, 2, 256), BF),
                pltpu.VMEM((4, 1024, 128), BF),
                pltpu.VMEM((2, 512, 128), F32),
                pltpu.VMEM((256, 2, 128), F32),
                pltpu.VMEM((256, 2, 128), F32),
                pltpu.SemaphoreType.REGULAR((8,)),
                pltpu.SemaphoreType.DMA((2,)),
                pltpu.SemaphoreType.DMA((2,)),
                pltpu.SemaphoreType.DMA((2,)),
                pltpu.SemaphoreType.DMA((2,)),
                pltpu.SemaphoreType.DMA((2,)),
            ],
            compiler_params=pltpu.CompilerParams(collective_id=0, has_side_effects=True),
        )(voltages[0, 0], jnp.swapaxes(weights, 3, 4))
        out = pl.pallas_call(
            layout_kernel,
            out_shape=jax.ShapeDtypeStruct((2, 4, 32, 256), F32),
            in_specs=[vmem],
            out_specs=vmem,
        )(got)
        return jnp.transpose(out, (3, 0, 1, 2))

    return jax.shard_map(
        on_device,
        mesh=mesh,
        in_specs=(P("ta", "gx", None, None, None), P(None, "gx", None, None, None)),
        out_specs=P(None, None, "gx", "ta"),
        check_vma=False,
    )
```

```python
import jax
import jax.numpy as jnp
from jax import lax
from jax.experimental import pallas as pl
from jax.experimental.pallas import tpu as pltpu
from jax.sharding import PartitionSpec as P

MESH = pl.DeviceIdType.MESH
BF = jnp.bfloat16
F32 = jnp.float32
NX, NY, NZ, NC = 4, 4, 8, 2


def iota(shape, dim):
    return lax.broadcasted_iota(jnp.int32, shape, dim)


def one_hot(cond):
    return jnp.where(cond, 1.0, 0.0).astype(BF)


def dot(a, b):
    return jnp.dot(a, b, preferred_element_type=F32)


def tn_dot(a, b):
    return lax.dot_general(a, b, (((0,), (0,)), ((), ())), preferred_element_type=F32)


def exchange_kernel(x_hbm, w_hbm, out_ref, xv, wv, snd, rcv, amat, acc, snd2,
                    line_sem, in_sem, send_sem, recv_sem, send2_sem, recv2_sem):
    ta = lax.axis_index("ta")
    g = lax.axis_index("gx")
    core = lax.rem(g, 2)
    y = lax.rem(lax.div(g, 2), NY)
    z = lax.rem(lax.div(g, 8), NZ)
    x_lo = lax.div(g, 64)
    x = ta * 2 + x_lo
    me = ta * 128 + g
    copy_x = pltpu.make_async_copy(x_hbm, xv, in_sem.at[0])
    copy_w = pltpu.make_async_copy(w_hbm, wv, in_sem.at[1])
    copy_x.start()
    copy_w.start()

    nxs = [lax.rem(x + d, NX) for d in range(NX)]
    tas = [lax.div(v, 2) for v in nxs]
    xbs = [lax.rem(v, 2) * 64 for v in nxs]
    ybs = [lax.rem(y + d, NY) * 2 for d in range(NY)]
    zbs = [lax.rem(z + d, NZ) * 8 for d in range(NZ)]
    cores = [core, 1 - core]
    far_z = (4, 3, 5, 2, 6, 1, 7, 0)

    def signal(sem, nta, ng):
        pl.semaphore_signal(sem, inc=1, device_id={"ta": nta, "gx": ng}, device_id_type=MESH)

    barrier = pltpu.get_barrier_semaphore()
    corner = x_lo * 64 + y * 2
    line = [corner + zbs[dz] + cores[dc] for dz in far_z for dc in (1, 0)]
    others = [(dx, dy) for dx in (2, 1, 3, 0) for dy in (2, 1, 3, 0)][:-1]
    for ng in line[:-1]:
        signal(barrier, ta, ng)
    for dx, dy in others:
        signal(barrier, tas[dx], xbs[dx] + ybs[dy] + zbs[0] + core)

    copy_x.wait()
    r_i, r_k = iota((128, 128), 0), iota((128, 128), 1)
    rows = one_hot(r_k == (r_i & 1) * 64 + ((r_i >> 1) & 31) * 2 + (r_i >> 6))
    p_i, p_k = iota((256, 256), 0), iota((256, 256), 1)
    lanes = one_hot(p_i == (p_k & 31) * 8 + (p_k >> 5))
    snd_rows = snd.reshape(1024, 256)
    for blk in range(4):
        block = jnp.concatenate([xv[0, blk * 64:(blk + 1) * 64], xv[1, blk * 64:(blk + 1) * 64]], 0)
        grouped = dot(rows, block).astype(BF)
        for h in range(2):
            piece = dot(grouped[:, h * 256:(h + 1) * 256], lanes).astype(BF)
            for j in range(2):
                snd_rows[pl.ds(j * 512 + h * 256 + blk * 64, 64), :] = piece[j * 64:(j + 1) * 64]

    pl.semaphore_wait(barrier, 30)
    for dx, dy in others:
        signal(line_sem.at[x * 4 + y], tas[dx], xbs[dx] + ybs[dy] + zbs[0] + core)

    def send(j, nta, ng):
        pltpu.make_async_remote_copy(
            snd.at[j * 256 + nta * 128 + ng], rcv.at[j * 256 + me], send_sem.at[j], recv_sem.at[j],
            device_id={"ta": nta, "gx": ng}, device_id_type=MESH).start()

    def send_own(j):
        for ng in line[:-1]:
            send(j, ta, ng)
        rcv[j * 256 + me] = snd[j * 256 + me]

    def send_line(j, wait):
        def step(i, carry):
            nx = lax.rem(x + lax.rem(i, NX), NX)
            ny = lax.rem(y + lax.div(i, NX), NY)
            if wait:
                pl.semaphore_wait(line_sem.at[nx * 4 + ny], 1)
            nta = lax.div(nx, 2)
            base = lax.rem(nx, 2) * 64 + ny * 2
            for dz in far_z:
                for dc in (1, 0):
                    send(j, nta, base + zbs[dz] + cores[dc])
            return carry
        return step

    send_own(0)
    lax.fori_loop(1, 16, send_line(0, True), 0)
    send_own(1)
    lax.fori_loop(1, 16, send_line(1, False), 0)

    copy_w.wait()
    b_i, b_k = iota((512, 512), 0), iota((512, 512), 1)
    beams = one_hot(b_i == (b_k & 255) * 2 + (b_k >> 8))
    e_i, e_k = iota((128, 256), 0), iota((128, 256), 1)
    e_ri, e_a = e_i >> 6, e_i & 63
    k_c, k_a, k_ri = e_k >> 7, (e_k >> 1) & 63, e_k & 1
    sign = jnp.where((k_c == 0) & (k_ri == 1), -1.0, 1.0)
    spread = jnp.where((e_a == k_a) & (e_ri == (k_c ^ k_ri)), sign, 0.0).astype(BF)
    for j in range(2):
        for q in range(2):
            both = dot(wv[q, j].reshape(128, 512), beams).astype(BF)
            made = tn_dot(both, spread).astype(BF)
            amat[j * 2 + q, 0:512, :] = made[:, 0:128]
            amat[j * 2 + q, 512:1024, :] = made[:, 128:256]

    rcv_rows = rcv.reshape(1024, 256)
    lane = iota((256, 128), 1)
    low, even = lane < 64, (lane & 32) == 0

    def send2(j, ng):
        pltpu.make_async_remote_copy(
            snd2.at[j * 128 + ng], out_ref.at[j * 128 + g], send2_sem.at[j], recv2_sem.at[j],
            device_id={"ta": ta, "gx": ng}, device_id_type=MESH).start()

    half_plane = [lax.rem(x_lo + dx, 2) * 64 + ybs[dy] + cores[dc]
                  for dx in (1, 0) for dy in (2, 1, 3, 0) for dc in (1, 0)]

    for j in range(2):
        pltpu.make_async_copy(snd.at[pl.ds(0, 255)], rcv.at[pl.ds(0, 255)], recv_sem.at[j]).wait()

        def channel(q, carry):
            total = None
            for h in range(2):
                start = pl.multiple_of(j * 512 + h * 256 + q * 128, 128)
                field = dot(amat[j * 2 + q], rcv_rows[pl.ds(start, 128), :])
                re, im = field[0:512], field[512:1024]
                power = re * re + im * im
                part = power[:, 0:128] + power[:, 128:256]
                total = part if total is None else total + part
            acc[q] = total
            return carry

        lax.fori_loop(0, 2, channel, 0)
        fold = []
        for q in range(2):
            a, b = acc[q, 0:256], acc[q, 256:512]
            fold.append(jnp.where(low, a, b) + pltpu.roll(jnp.where(low, b, a), 64, 1))
        other = jnp.where(even, fold[1], fold[0])
        summed = jnp.where(even, fold[0], fold[1]) + jnp.where(
            even, pltpu.roll(other, 96, 1), pltpu.roll(other, 32, 1))
        snd2.reshape(512, 128)[j * 256:(j + 1) * 256, :] = summed

        def send2_step(i, carry):
            far = 4 + (2 * lax.rem(i, 2) - 1) * lax.div(i, 2)
            zz = lax.rem(z + far, NZ)
            for base in half_plane:
                send2(j, base + zz * 8)
            return carry

        lax.fori_loop(1, NZ, send2_step, 0)
        for base in half_plane[:-1]:
            send2(j, base + z * 8)
        out_ref[j * 128 + g] = snd2[j * 128 + g]

    for j in range(2):
        pltpu.make_async_copy(snd2.at[pl.ds(0, 127)], out_ref.at[pl.ds(0, 127)], recv2_sem.at[j]).wait()
    for j in range(2):
        pltpu.make_async_copy(snd.at[pl.ds(0, 255)], rcv.at[pl.ds(0, 255)], send_sem.at[j]).wait()
        pltpu.make_async_copy(snd2.at[pl.ds(0, 127)], out_ref.at[pl.ds(0, 127)], send2_sem.at[j]).wait()


def layout_kernel(r_ref, out_ref):
    lane = iota((32, 128), 1)
    half = lane >> 1
    odd = (lane & 1) == 1
    for high in range(2):
        turned = [r_ref[j * 128:(j + 1) * 128, high, :].T for j in range(2)]
        for parity in range(2):
            for q in range(2):
                at = parity * 64 + q * 32
                for part in range(2):
                    index = half + part * 64
                    out_ref[q, high * 2 + parity, :, part * 128:(part + 1) * 128] = jnp.where(
                        odd, jnp.take_along_axis(turned[1][at:at + 32], index, axis=1),
                        jnp.take_along_axis(turned[0][at:at + 32], index, axis=1))


def solution(mesh):
    def on_device(voltages, weights):
        vmem = pl.BlockSpec(memory_space=pltpu.VMEM)
        hbm = pl.BlockSpec(memory_space=pl.ANY)
        got = pl.pallas_call(
            exchange_kernel,
            out_shape=pltpu.VMEM((256, 2, 128), F32),
            in_specs=[hbm, hbm],
            out_specs=vmem,
            scratch_shapes=[
                pltpu.VMEM((2, 256, 512), BF),
                pltpu.VMEM((2, 2, 2, 64, 512), BF),
                pltpu.VMEM((512, 2, 256), BF),
                pltpu.VMEM((512, 2, 256), BF),
                pltpu.VMEM((4, 1024, 128), BF),
                pltpu.VMEM((2, 512, 128), F32),
                pltpu.VMEM((256, 2, 128), F32),
                pltpu.SemaphoreType.REGULAR((16,)),
                pltpu.SemaphoreType.DMA((2,)),
                pltpu.SemaphoreType.DMA((2,)),
                pltpu.SemaphoreType.DMA((2,)),
                pltpu.SemaphoreType.DMA((2,)),
                pltpu.SemaphoreType.DMA((2,)),
            ],
            compiler_params=pltpu.CompilerParams(collective_id=0, has_side_effects=True),
        )(voltages[0, 0], jnp.swapaxes(weights, 3, 4))
        out = pl.pallas_call(
            layout_kernel,
            out_shape=jax.ShapeDtypeStruct((2, 4, 32, 256), F32),
            in_specs=[vmem],
            out_specs=vmem,
            compiler_params=pltpu.CompilerParams(vmem_limit_bytes=8 * 2**20),
        )(got)
        return jnp.transpose(out, (3, 0, 1, 2))

    return jax.shard_map(
        on_device,
        mesh=mesh,
        in_specs=(P("ta", "gx", None, None, None), P(None, "gx", None, None, None)),
        out_specs=P(None, None, "gx", "ta"),
        check_vma=False,
    )
```

```python
import jax
import jax.numpy as jnp
from jax import lax
from jax.experimental import pallas as pl
from jax.experimental.pallas import tpu as pltpu
from jax.sharding import PartitionSpec as P

MESH = pl.DeviceIdType.MESH
BF = jnp.bfloat16
F32 = jnp.float32
NX, NY, NZ, NC = 4, 4, 8, 2


def iota(shape, dim):
    return lax.broadcasted_iota(jnp.int32, shape, dim)


def one_hot(cond):
    return jnp.where(cond, 1.0, 0.0).astype(BF)


def dot(a, b):
    return jnp.dot(a, b, preferred_element_type=F32)


def tn_dot(a, b):
    return lax.dot_general(a, b, (((0,), (0,)), ((), ())), preferred_element_type=F32)


def exchange_kernel(x_hbm, w_hbm, out_ref, xv, wv, snd, rcv, amat, acc, snd2,
                    line_sem, in_sem, send_sem, recv_sem, send2_sem, recv2_sem):
    ta = lax.axis_index("ta")
    g = lax.axis_index("gx")
    core = lax.rem(g, 2)
    y = lax.rem(lax.div(g, 2), NY)
    z = lax.rem(lax.div(g, 8), NZ)
    x_lo = lax.div(g, 64)
    x = ta * 2 + x_lo
    me = ta * 128 + g
    copy_x = pltpu.make_async_copy(x_hbm, xv, in_sem.at[0])
    copy_w = pltpu.make_async_copy(w_hbm, wv, in_sem.at[1])
    copy_x.start()
    copy_w.start()

    nxs = [lax.rem(x + d, NX) for d in range(NX)]
    tas = [lax.div(v, 2) for v in nxs]
    xbs = [lax.rem(v, 2) * 64 for v in nxs]
    ybs = [lax.rem(y + d, NY) * 2 for d in range(NY)]
    zbs = [lax.rem(z + d, NZ) * 8 for d in range(NZ)]
    cores = [core, 1 - core]
    far_z = (4, 3, 5, 2, 6, 1, 7, 0)

    def signal(sem, nta, ng):
        pl.semaphore_signal(sem, inc=1, device_id={"ta": nta, "gx": ng}, device_id_type=MESH)

    barrier = pltpu.get_barrier_semaphore()
    corner = x_lo * 64 + y * 2
    line = [corner + zbs[dz] + cores[dc] for dz in far_z for dc in (1, 0)]
    others = [(dx, dy) for dx in (2, 1, 3, 0) for dy in (2, 1, 3, 0)][:-1]
    for ng in line[:-1]:
        signal(barrier, ta, ng)
    for dx, dy in others:
        signal(barrier, tas[dx], xbs[dx] + ybs[dy] + zbs[0] + core)

    copy_x.wait()
    r_i, r_k = iota((128, 128), 0), iota((128, 128), 1)
    rows = one_hot(r_k == (r_i & 1) * 64 + ((r_i >> 1) & 31) * 2 + (r_i >> 6))
    p_i, p_k = iota((256, 256), 0), iota((256, 256), 1)
    lanes = one_hot(p_i == (p_k & 31) * 8 + (p_k >> 5))
    snd_rows = snd.reshape(1024, 256)
    for blk in range(4):
        block = jnp.concatenate([xv[0, blk * 64:(blk + 1) * 64], xv[1, blk * 64:(blk + 1) * 64]], 0)
        grouped = dot(rows, block).astype(BF)
        for h in range(2):
            piece = dot(grouped[:, h * 256:(h + 1) * 256], lanes).astype(BF)
            for j in range(2):
                snd_rows[pl.ds(j * 512 + h * 256 + blk * 64, 64), :] = piece[j * 64:(j + 1) * 64]

    pl.semaphore_wait(barrier, 30)
    for dx, dy in others:
        signal(line_sem.at[x * 4 + y], tas[dx], xbs[dx] + ybs[dy] + zbs[0] + core)

    def send(j, nta, ng):
        pltpu.make_async_remote_copy(
            snd.at[j * 256 + nta * 128 + ng], rcv.at[j * 256 + me], send_sem.at[j], recv_sem.at[j],
            device_id={"ta": nta, "gx": ng}, device_id_type=MESH).start()

    def send_own(j):
        for ng in line[:-1]:
            send(j, ta, ng)
        rcv[j * 256 + me] = snd[j * 256 + me]

    def send_line(j, wait):
        def step(i, carry):
            nx = lax.div(i, 8) * 2 + lax.rem(x + i, 2)
            ny = lax.rem(y + lax.div(lax.rem(i, 8), 2), NY)

            @pl.when((nx != x) | (ny != y))
            def _():
                if wait:
                    pl.semaphore_wait(line_sem.at[nx * 4 + ny], 1)
                nta = lax.div(nx, 2)
                base = lax.rem(nx, 2) * 64 + ny * 2
                for dz in far_z:
                    for dc in (1, 0):
                        send(j, nta, base + zbs[dz] + cores[dc])
            return carry
        return step

    send_own(0)
    lax.fori_loop(0, 16, send_line(0, True), 0)
    send_own(1)
    lax.fori_loop(0, 16, send_line(1, False), 0)

    copy_w.wait()
    b_i, b_k = iota((512, 512), 0), iota((512, 512), 1)
    beams = one_hot(b_i == (b_k & 255) * 2 + (b_k >> 8))
    e_i, e_k = iota((128, 256), 0), iota((128, 256), 1)
    e_ri, e_a = e_i >> 6, e_i & 63
    k_c, k_a, k_ri = e_k >> 7, (e_k >> 1) & 63, e_k & 1
    sign = jnp.where((k_c == 0) & (k_ri == 1), -1.0, 1.0)
    spread = jnp.where((e_a == k_a) & (e_ri == (k_c ^ k_ri)), sign, 0.0).astype(BF)
    for j in range(2):
        for q in range(2):
            both = dot(wv[q, j].reshape(128, 512), beams).astype(BF)
            made = tn_dot(both, spread).astype(BF)
            amat[j * 2 + q, 0:512, :] = made[:, 0:128]
            amat[j * 2 + q, 512:1024, :] = made[:, 128:256]

    rcv_rows = rcv.reshape(1024, 256)
    lane = iota((256, 128), 1)
    low, even = lane < 64, (lane & 32) == 0

    def send2(j, ng):
        pltpu.make_async_remote_copy(
            snd2.at[j * 128 + ng], out_ref.at[j * 128 + g], send2_sem.at[j], recv2_sem.at[j],
            device_id={"ta": ta, "gx": ng}, device_id_type=MESH).start()

    half_plane = [lax.rem(x_lo + dx, 2) * 64 + ybs[dy] + cores[dc]
                  for dx in (1, 0) for dy in (2, 1, 3, 0) for dc in (1, 0)]

    for j in range(2):
        pltpu.make_async_copy(snd.at[pl.ds(0, 255)], rcv.at[pl.ds(0, 255)], recv_sem.at[j]).wait()

        def channel(q, carry):
            total = None
            for h in range(2):
                start = pl.multiple_of(j * 512 + h * 256 + q * 128, 128)
                field = dot(amat[j * 2 + q], rcv_rows[pl.ds(start, 128), :])
                re, im = field[0:512], field[512:1024]
                power = re * re + im * im
                part = power[:, 0:128] + power[:, 128:256]
                total = part if total is None else total + part
            acc[q] = total
            return carry

        lax.fori_loop(0, 2, channel, 0)
        fold = []
        for q in range(2):
            a, b = acc[q, 0:256], acc[q, 256:512]
            fold.append(jnp.where(low, a, b) + pltpu.roll(jnp.where(low, b, a), 64, 1))
        other = jnp.where(even, fold[1], fold[0])
        summed = jnp.where(even, fold[0], fold[1]) + jnp.where(
            even, pltpu.roll(other, 96, 1), pltpu.roll(other, 32, 1))
        snd2.reshape(512, 128)[j * 256:(j + 1) * 256, :] = summed

        def send2_step(i, carry):
            far = 4 + (2 * lax.rem(i, 2) - 1) * lax.div(i, 2)
            zz = lax.rem(z + far, NZ)
            for base in half_plane:
                send2(j, base + zz * 8)
            return carry

        lax.fori_loop(1, NZ, send2_step, 0)
        for base in half_plane[:-1]:
            send2(j, base + z * 8)
        out_ref[j * 128 + g] = snd2[j * 128 + g]

    for j in range(2):
        pltpu.make_async_copy(snd2.at[pl.ds(0, 127)], out_ref.at[pl.ds(0, 127)], recv2_sem.at[j]).wait()
    for j in range(2):
        pltpu.make_async_copy(snd.at[pl.ds(0, 255)], rcv.at[pl.ds(0, 255)], send_sem.at[j]).wait()
        pltpu.make_async_copy(snd2.at[pl.ds(0, 127)], out_ref.at[pl.ds(0, 127)], send2_sem.at[j]).wait()


def layout_kernel(r_ref, out_ref):
    lane = iota((32, 128), 1)
    half = lane >> 1
    odd = (lane & 1) == 1
    for high in range(2):
        turned = [r_ref[j * 128:(j + 1) * 128, high, :].T for j in range(2)]
        for parity in range(2):
            for q in range(2):
                at = parity * 64 + q * 32
                for part in range(2):
                    index = half + part * 64
                    out_ref[q, high * 2 + parity, :, part * 128:(part + 1) * 128] = jnp.where(
                        odd, jnp.take_along_axis(turned[1][at:at + 32], index, axis=1),
                        jnp.take_along_axis(turned[0][at:at + 32], index, axis=1))


def solution(mesh):
    def on_device(voltages, weights):
        vmem = pl.BlockSpec(memory_space=pltpu.VMEM)
        hbm = pl.BlockSpec(memory_space=pl.ANY)
        got = pl.pallas_call(
            exchange_kernel,
            out_shape=pltpu.VMEM((256, 2, 128), F32),
            in_specs=[hbm, hbm],
            out_specs=vmem,
            scratch_shapes=[
                pltpu.VMEM((2, 256, 512), BF),
                pltpu.VMEM((2, 2, 2, 64, 512), BF),
                pltpu.VMEM((512, 2, 256), BF),
                pltpu.VMEM((512, 2, 256), BF),
                pltpu.VMEM((4, 1024, 128), BF),
                pltpu.VMEM((2, 512, 128), F32),
                pltpu.VMEM((256, 2, 128), F32),
                pltpu.SemaphoreType.REGULAR((16,)),
                pltpu.SemaphoreType.DMA((2,)),
                pltpu.SemaphoreType.DMA((2,)),
                pltpu.SemaphoreType.DMA((2,)),
                pltpu.SemaphoreType.DMA((2,)),
                pltpu.SemaphoreType.DMA((2,)),
            ],
            compiler_params=pltpu.CompilerParams(collective_id=0, has_side_effects=True),
        )(voltages[0, 0], jnp.swapaxes(weights, 3, 4))
        out = pl.pallas_call(
            layout_kernel,
            out_shape=jax.ShapeDtypeStruct((2, 4, 32, 256), F32),
            in_specs=[vmem],
            out_specs=vmem,
            compiler_params=pltpu.CompilerParams(vmem_limit_bytes=8 * 2**20),
        )(got)
        return jnp.transpose(out, (3, 0, 1, 2))

    return jax.shard_map(
        on_device,
        mesh=mesh,
        in_specs=(P("ta", "gx", None, None, None), P(None, "gx", None, None, None)),
        out_specs=P(None, None, "gx", "ta"),
        check_vma=False,
    )
```

```python
import jax
import jax.numpy as jnp
from jax import lax
from jax.experimental import pallas as pl
from jax.experimental.pallas import tpu as pltpu
from jax.sharding import PartitionSpec as P

MESH = pl.DeviceIdType.MESH
BF = jnp.bfloat16
F32 = jnp.float32
NX, NY, NZ, NC = 4, 4, 8, 2


def iota(shape, dim):
    return lax.broadcasted_iota(jnp.int32, shape, dim)


def one_hot(cond):
    return jnp.where(cond, 1.0, 0.0).astype(BF)


def dot(a, b):
    return jnp.dot(a, b, preferred_element_type=F32)


def tn_dot(a, b):
    return lax.dot_general(a, b, (((0,), (0,)), ((), ())), preferred_element_type=F32)


def exchange_kernel(x_hbm, w_hbm, out_ref, xv, wv, snd, rcv, amat, acc, snd2,
                    line_sem, in_sem, send_sem, recv_sem, send2_sem, recv2_sem):
    ta = lax.axis_index("ta")
    g = lax.axis_index("gx")
    core = lax.rem(g, 2)
    y = lax.rem(lax.div(g, 2), NY)
    z = lax.rem(lax.div(g, 8), NZ)
    x_lo = lax.div(g, 64)
    x = ta * 2 + x_lo
    me = ta * 128 + g
    copy_x = pltpu.make_async_copy(x_hbm, xv, in_sem.at[0])
    copy_w = pltpu.make_async_copy(w_hbm, wv, in_sem.at[1])
    copy_x.start()
    copy_w.start()

    nxs = [lax.rem(x + d, NX) for d in range(NX)]
    tas = [lax.div(v, 2) for v in nxs]
    xbs = [lax.rem(v, 2) * 64 for v in nxs]
    ybs = [lax.rem(y + d, NY) * 2 for d in range(NY)]
    zbs = [lax.rem(z + d, NZ) * 8 for d in range(NZ)]
    cores = [core, 1 - core]
    far_z = (4, 3, 5, 2, 6, 1, 7, 0)

    def signal(sem, nta, ng):
        pl.semaphore_signal(sem, inc=1, device_id={"ta": nta, "gx": ng}, device_id_type=MESH)

    barrier = pltpu.get_barrier_semaphore()
    corner = x_lo * 64 + y * 2
    line = [corner + zbs[dz] + cores[dc] for dz in far_z for dc in (1, 0)]
    others = [(dx, dy) for dx in (2, 1, 3, 0) for dy in (2, 1, 3, 0)][:-1]
    for ng in line[:-1]:
        signal(barrier, ta, ng)
    for dx, dy in others:
        signal(barrier, tas[dx], xbs[dx] + ybs[dy] + zbs[0] + core)

    r_i, r_k = iota((64, 128), 0), iota((64, 128), 1)
    picked = (r_i & 1) * 64 + (r_i >> 1) * 2
    p_i, p_k = iota((256, 256), 0), iota((256, 256), 1)
    lanes = one_hot(p_i == (p_k & 31) * 8 + (p_k >> 5))
    snd_rows = snd.reshape(1024, 256)

    def prepare(j):
        rows = one_hot(r_k == picked + j)
        grouped = []
        for blk in range(4):
            block = jnp.concatenate([xv[0, blk * 64:(blk + 1) * 64], xv[1, blk * 64:(blk + 1) * 64]], 0)
            grouped.append(dot(rows, block).astype(BF))
        grouped = jnp.concatenate(grouped, 0)
        for h in range(2):
            snd_rows[j * 512 + h * 256:j * 512 + h * 256 + 256, :] = dot(
                grouped[:, h * 256:(h + 1) * 256], lanes).astype(BF)

    copy_x.wait()
    prepare(0)
    prepare(1)
    pl.semaphore_wait(barrier, 30)
    for dx, dy in others:
        signal(line_sem.at[x * 4 + y], tas[dx], xbs[dx] + ybs[dy] + zbs[0] + core)

    def send(j, nta, ng):
        pltpu.make_async_remote_copy(
            snd.at[j * 256 + nta * 128 + ng], rcv.at[j * 256 + me], send_sem.at[j], recv_sem.at[j * 2 + ta],
            device_id={"ta": nta, "gx": ng}, device_id_type=MESH).start()

    def send_own(j):
        for ng in line[:-1]:
            send(j, ta, ng)
        rcv[j * 256 + me] = snd[j * 256 + me]

    def send_line(j, wait):
        def step(i, carry):
            nx = lax.div(i, 8) * 2 + lax.rem(x + i, 2)
            ny = lax.rem(y + lax.div(lax.rem(i, 8), 2), NY)

            @pl.when((nx != x) | (ny != y))
            def _():
                if wait:
                    pl.semaphore_wait(line_sem.at[nx * 4 + ny], 1)
                nta = lax.div(nx, 2)
                base = lax.rem(nx, 2) * 64 + ny * 2
                for dz in far_z:
                    for dc in (1, 0):
                        send(j, nta, base + zbs[dz] + cores[dc])
            return carry
        return step

    send_own(0)
    lax.fori_loop(0, 16, send_line(0, True), 0)
    send_own(1)
    lax.fori_loop(0, 16, send_line(1, False), 0)

    copy_w.wait()
    b_i, b_k = iota((512, 512), 0), iota((512, 512), 1)
    beams = one_hot(b_i == (b_k & 255) * 2 + (b_k >> 8))
    e_i, e_k = iota((128, 256), 0), iota((128, 256), 1)
    e_ri, e_a = e_i >> 6, e_i & 63
    k_c, k_a, k_ri = e_k >> 7, (e_k >> 1) & 63, e_k & 1
    sign = jnp.where((k_c == 0) & (k_ri == 1), -1.0, 1.0)
    spread = jnp.where((e_a == k_a) & (e_ri == (k_c ^ k_ri)), sign, 0.0).astype(BF)
    for j in range(2):
        for q in range(2):
            both = dot(wv[q, j].reshape(128, 512), beams).astype(BF)
            made = tn_dot(both, spread).astype(BF)
            amat[j * 2 + q, 0:512, :] = made[:, 0:128]
            amat[j * 2 + q, 512:1024, :] = made[:, 128:256]

    rcv_rows = rcv.reshape(1024, 256)
    lane = iota((256, 128), 1)
    low, even = lane < 64, (lane & 32) == 0

    def send2(j, ng):
        pltpu.make_async_remote_copy(
            snd2.at[j * 128 + ng], out_ref.at[j * 128 + g], send2_sem.at[j], recv2_sem.at[j],
            device_id={"ta": ta, "gx": ng}, device_id_type=MESH).start()

    half_plane = [lax.rem(x_lo + dx, 2) * 64 + ybs[dy] + cores[dc]
                  for dx in (1, 0) for dy in (2, 1, 3, 0) for dc in (1, 0)]

    for j in range(2):
        for step in range(2):
            h = ta if step == 0 else 1 - ta
            n = 127 + step
            pltpu.make_async_copy(snd.at[pl.ds(0, n)], rcv.at[pl.ds(0, n)], recv_sem.at[j * 2 + h]).wait()
            for q in range(2):
                start = pl.multiple_of(j * 512 + h * 256 + q * 128, 128)
                field = dot(amat[j * 2 + q], rcv_rows[pl.ds(start, 128), :])
                re, im = field[0:512], field[512:1024]
                power = re * re + im * im
                part = power[:, 0:128] + power[:, 128:256]
                acc[q] = part if step == 0 else acc[q] + part

        fold = []
        for q in range(2):
            a, b = acc[q, 0:256], acc[q, 256:512]
            fold.append(jnp.where(low, a, b) + pltpu.roll(jnp.where(low, b, a), 64, 1))
        other = jnp.where(even, fold[1], fold[0])
        summed = jnp.where(even, fold[0], fold[1]) + jnp.where(
            even, pltpu.roll(other, 96, 1), pltpu.roll(other, 32, 1))
        snd2.reshape(512, 128)[j * 256:(j + 1) * 256, :] = summed

        def send2_step(i, carry):
            far = 4 + (2 * lax.rem(i, 2) - 1) * lax.div(i, 2)
            zz = lax.rem(z + far, NZ)
            for base in half_plane:
                send2(j, base + zz * 8)
            return carry

        lax.fori_loop(1, NZ, send2_step, 0)
        for base in half_plane[:-1]:
            send2(j, base + z * 8)
        out_ref[j * 128 + g] = snd2[j * 128 + g]

    for j in range(2):
        pltpu.make_async_copy(snd2.at[pl.ds(0, 127)], out_ref.at[pl.ds(0, 127)], recv2_sem.at[j]).wait()
    for j in range(2):
        pltpu.make_async_copy(snd.at[pl.ds(0, 255)], rcv.at[pl.ds(0, 255)], send_sem.at[j]).wait()
        pltpu.make_async_copy(snd2.at[pl.ds(0, 127)], out_ref.at[pl.ds(0, 127)], send2_sem.at[j]).wait()


def layout_kernel(r_ref, out_ref):
    lane = iota((32, 128), 1)
    half = lane >> 1
    odd = (lane & 1) == 1
    for high in range(2):
        turned = [r_ref[j * 128:(j + 1) * 128, high, :].T for j in range(2)]
        for parity in range(2):
            for q in range(2):
                at = parity * 64 + q * 32
                for part in range(2):
                    index = half + part * 64
                    out_ref[q, high * 2 + parity, :, part * 128:(part + 1) * 128] = jnp.where(
                        odd, jnp.take_along_axis(turned[1][at:at + 32], index, axis=1),
                        jnp.take_along_axis(turned[0][at:at + 32], index, axis=1))


def solution(mesh):
    def on_device(voltages, weights):
        vmem = pl.BlockSpec(memory_space=pltpu.VMEM)
        hbm = pl.BlockSpec(memory_space=pl.ANY)
        got = pl.pallas_call(
            exchange_kernel,
            out_shape=pltpu.VMEM((256, 2, 128), F32),
            in_specs=[hbm, hbm],
            out_specs=vmem,
            scratch_shapes=[
                pltpu.VMEM((2, 256, 512), BF),
                pltpu.VMEM((2, 2, 2, 64, 512), BF),
                pltpu.VMEM((512, 2, 256), BF),
                pltpu.VMEM((512, 2, 256), BF),
                pltpu.VMEM((4, 1024, 128), BF),
                pltpu.VMEM((2, 512, 128), F32),
                pltpu.VMEM((256, 2, 128), F32),
                pltpu.SemaphoreType.REGULAR((16,)),
                pltpu.SemaphoreType.DMA((2,)),
                pltpu.SemaphoreType.DMA((2,)),
                pltpu.SemaphoreType.DMA((4,)),
                pltpu.SemaphoreType.DMA((2,)),
                pltpu.SemaphoreType.DMA((2,)),
            ],
            compiler_params=pltpu.CompilerParams(collective_id=0, has_side_effects=True),
        )(voltages[0, 0], jnp.swapaxes(weights, 3, 4))
        out = pl.pallas_call(
            layout_kernel,
            out_shape=jax.ShapeDtypeStruct((2, 4, 32, 256), F32),
            in_specs=[vmem],
            out_specs=vmem,
            compiler_params=pltpu.CompilerParams(vmem_limit_bytes=8 * 2**20),
        )(got)
        return jnp.transpose(out, (3, 0, 1, 2))

    return jax.shard_map(
        on_device,
        mesh=mesh,
        in_specs=(P("ta", "gx", None, None, None), P(None, "gx", None, None, None)),
        out_specs=P(None, None, "gx", "ta"),
        check_vma=False,
    )
```

```python
import jax
import jax.numpy as jnp
from jax import lax
from jax.experimental import pallas as pl
from jax.experimental.pallas import tpu as pltpu
from jax.sharding import PartitionSpec as P

MESH = pl.DeviceIdType.MESH
BF = jnp.bfloat16
F32 = jnp.float32
NX, NY, NZ, NC = 4, 4, 8, 2


def iota(shape, dim):
    return lax.broadcasted_iota(jnp.int32, shape, dim)


def one_hot(cond):
    return jnp.where(cond, 1.0, 0.0).astype(BF)


def dot(a, b):
    return jnp.dot(a, b, preferred_element_type=F32)


def tn_dot(a, b):
    return lax.dot_general(a, b, (((0,), (0,)), ((), ())), preferred_element_type=F32)


def exchange_kernel(x_hbm, w_hbm, out_ref, xv, wv, snd, rcv, amat, acc, snd2, rcv2,
                    line_sem, in_sem, send_sem, recv_sem, send2_sem, recv2_sem):
    ta = lax.axis_index("ta")
    g = lax.axis_index("gx")
    core = lax.rem(g, 2)
    y = lax.rem(lax.div(g, 2), NY)
    z = lax.rem(lax.div(g, 8), NZ)
    x_lo = lax.div(g, 64)
    x = ta * 2 + x_lo
    me = ta * 128 + g
    copy_x = pltpu.make_async_copy(x_hbm, xv, in_sem.at[0])
    copy_w = pltpu.make_async_copy(w_hbm, wv, in_sem.at[1])
    copy_x.start()
    copy_w.start()

    nxs = [lax.rem(x + d, NX) for d in range(NX)]
    tas = [lax.div(v, 2) for v in nxs]
    xbs = [lax.rem(v, 2) * 64 for v in nxs]
    ybs = [lax.rem(y + d, NY) * 2 for d in range(NY)]
    zbs = [lax.rem(z + d, NZ) * 8 for d in range(NZ)]
    cores = [core, 1 - core]
    far_z = (4, 3, 5, 2, 6, 1, 7, 0)

    def signal(sem, nta, ng):
        pl.semaphore_signal(sem, inc=1, device_id={"ta": nta, "gx": ng}, device_id_type=MESH)

    barrier = pltpu.get_barrier_semaphore()
    corner = x_lo * 64 + y * 2
    line = [corner + zbs[dz] + cores[dc] for dz in far_z for dc in (1, 0)]
    others = [(dx, dy) for dx in (2, 1, 3, 0) for dy in (2, 1, 3, 0)][:-1]
    for ng in line[:-1]:
        signal(barrier, ta, ng)
    for dx, dy in others:
        signal(barrier, tas[dx], xbs[dx] + ybs[dy] + zbs[0] + core)

    r_i, r_k = iota((64, 128), 0), iota((64, 128), 1)
    picked = (r_i & 1) * 64 + (r_i >> 1) * 2
    p_i, p_k = iota((256, 256), 0), iota((256, 256), 1)
    lanes = one_hot(p_i == (p_k & 31) * 8 + (p_k >> 5))
    snd_rows = snd.reshape(1024, 256)

    def prepare(j):
        rows = one_hot(r_k == picked + j)
        grouped = []
        for blk in range(4):
            block = jnp.concatenate([xv[0, blk * 64:(blk + 1) * 64], xv[1, blk * 64:(blk + 1) * 64]], 0)
            grouped.append(dot(rows, block).astype(BF))
        grouped = jnp.concatenate(grouped, 0)
        for h in range(2):
            snd_rows[j * 512 + h * 256:j * 512 + h * 256 + 256, :] = dot(
                grouped[:, h * 256:(h + 1) * 256], lanes).astype(BF)

    copy_x.wait()
    prepare(0)
    prepare(1)
    pl.semaphore_wait(barrier, 30)
    for dx, dy in others:
        signal(line_sem.at[x * 4 + y], tas[dx], xbs[dx] + ybs[dy] + zbs[0] + core)

    def send(j, nta, ng):
        pltpu.make_async_remote_copy(
            snd.at[j * 256 + nta * 128 + ng], rcv.at[j * 256 + me], send_sem.at[j], recv_sem.at[j * 2 + ta],
            device_id={"ta": nta, "gx": ng}, device_id_type=MESH).start()

    def send_own(j):
        for ng in line[:-1]:
            send(j, ta, ng)
        rcv[j * 256 + me] = snd[j * 256 + me]

    def send_line(j, wait):
        def step(i, carry):
            nx = lax.div(i, 8) * 2 + lax.rem(x + i, 2)
            ny = lax.rem(y + lax.div(lax.rem(i, 8), 2), NY)

            @pl.when((nx != x) | (ny != y))
            def _():
                if wait:
                    pl.semaphore_wait(line_sem.at[nx * 4 + ny], 1)
                nta = lax.div(nx, 2)
                base = lax.rem(nx, 2) * 64 + ny * 2
                for dz in far_z:
                    for dc in (1, 0):
                        send(j, nta, base + zbs[dz] + cores[dc])
            return carry
        return step

    send_own(0)
    lax.fori_loop(0, 16, send_line(0, True), 0)
    send_own(1)
    lax.fori_loop(0, 16, send_line(1, False), 0)

    copy_w.wait()
    b_i, b_k = iota((512, 512), 0), iota((512, 512), 1)
    beams = one_hot(b_i == (b_k & 255) * 2 + (b_k >> 8))
    e_i, e_k = iota((128, 256), 0), iota((128, 256), 1)
    e_ri, e_a = e_i >> 6, e_i & 63
    k_c, k_a, k_ri = e_k >> 7, (e_k >> 1) & 63, e_k & 1
    sign = jnp.where((k_c == 0) & (k_ri == 1), -1.0, 1.0)
    spread = jnp.where((e_a == k_a) & (e_ri == (k_c ^ k_ri)), sign, 0.0).astype(BF)
    for j in range(2):
        for q in range(2):
            both = dot(wv[q, j].reshape(128, 512), beams).astype(BF)
            made = tn_dot(both, spread).astype(BF)
            amat[j * 2 + q, 0:512, :] = made[:, 0:128]
            amat[j * 2 + q, 512:1024, :] = made[:, 128:256]

    rcv_rows = rcv.reshape(1024, 256)
    lane = iota((256, 128), 1)
    low, even = lane < 64, (lane & 32) == 0

    def send2(j, ng):
        pltpu.make_async_remote_copy(
            snd2.at[j * 128 + ng], rcv2.at[j * 128 + g], send2_sem.at[j], recv2_sem.at[j],
            device_id={"ta": ta, "gx": ng}, device_id_type=MESH).start()

    half_plane = [lax.rem(x_lo + dx, 2) * 64 + ybs[dy] + cores[dc]
                  for dx in (1, 0) for dy in (2, 1, 3, 0) for dc in (1, 0)]

    for j in range(2):
        for step in range(2):
            h = ta if step == 0 else 1 - ta
            n = 127 + step
            pltpu.make_async_copy(snd.at[pl.ds(0, n)], rcv.at[pl.ds(0, n)], recv_sem.at[j * 2 + h]).wait()
            for q in range(2):
                start = pl.multiple_of(j * 512 + h * 256 + q * 128, 128)
                field = dot(amat[j * 2 + q], rcv_rows[pl.ds(start, 128), :])
                re, im = field[0:512], field[512:1024]
                power = re * re + im * im
                part = power[:, 0:128] + power[:, 128:256]
                acc[q] = part if step == 0 else acc[q] + part

        fold = []
        for q in range(2):
            a, b = acc[q, 0:256], acc[q, 256:512]
            fold.append(jnp.where(low, a, b) + pltpu.roll(jnp.where(low, b, a), 64, 1))
        other = jnp.where(even, fold[1], fold[0])
        summed = jnp.where(even, fold[0], fold[1]) + jnp.where(
            even, pltpu.roll(other, 96, 1), pltpu.roll(other, 32, 1))
        snd2.reshape(512, 128)[j * 256:(j + 1) * 256, :] = summed

        def send2_step(i, carry):
            far = 4 + (2 * lax.rem(i, 2) - 1) * lax.div(i, 2)
            zz = lax.rem(z + far, NZ)
            for base in half_plane:
                send2(j, base + zz * 8)
            return carry

        lax.fori_loop(1, NZ, send2_step, 0)
        for base in half_plane[:-1]:
            send2(j, base + z * 8)
        rcv2[j * 128 + g] = snd2[j * 128 + g]

    wide = iota((32, 128), 1)
    odd = (wide & 1) == 1

    def place(j):
        for high in range(2):
            turned = rcv2[j * 128:(j + 1) * 128, high, :].T
            for parity in range(2):
                for q in range(2):
                    at = parity * 64 + q * 32
                    for part in range(2):
                        cols = slice(part * 128, (part + 1) * 128)
                        own = jnp.take_along_axis(turned[at:at + 32], (wide >> 1) + part * 64, axis=1)
                        if j == 0:
                            out_ref[q, high * 2 + parity, :, cols] = own
                        else:
                            out_ref[q, high * 2 + parity, :, cols] = jnp.where(
                                odd, own, out_ref[q, high * 2 + parity, :, cols])

    for j in range(2):
        pltpu.make_async_copy(snd2.at[pl.ds(0, 127)], rcv2.at[pl.ds(0, 127)], recv2_sem.at[j]).wait()
        place(j)
    for j in range(2):
        pltpu.make_async_copy(snd.at[pl.ds(0, 255)], rcv.at[pl.ds(0, 255)], send_sem.at[j]).wait()
        pltpu.make_async_copy(snd2.at[pl.ds(0, 127)], rcv2.at[pl.ds(0, 127)], send2_sem.at[j]).wait()


def solution(mesh):
    def on_device(voltages, weights):
        vmem = pl.BlockSpec(memory_space=pltpu.VMEM)
        hbm = pl.BlockSpec(memory_space=pl.ANY)
        got = pl.pallas_call(
            exchange_kernel,
            out_shape=pltpu.VMEM((2, 4, 32, 256), F32),
            in_specs=[hbm, hbm],
            out_specs=vmem,
            scratch_shapes=[
                pltpu.VMEM((2, 256, 512), BF),
                pltpu.VMEM((2, 2, 2, 64, 512), BF),
                pltpu.VMEM((512, 2, 256), BF),
                pltpu.VMEM((512, 2, 256), BF),
                pltpu.VMEM((4, 1024, 128), BF),
                pltpu.VMEM((2, 512, 128), F32),
                pltpu.VMEM((256, 2, 128), F32),
                pltpu.VMEM((256, 2, 128), F32),
                pltpu.SemaphoreType.REGULAR((16,)),
                pltpu.SemaphoreType.DMA((2,)),
                pltpu.SemaphoreType.DMA((2,)),
                pltpu.SemaphoreType.DMA((4,)),
                pltpu.SemaphoreType.DMA((2,)),
                pltpu.SemaphoreType.DMA((2,)),
            ],
            compiler_params=pltpu.CompilerParams(collective_id=0, has_side_effects=True),
        )(voltages[0, 0], jnp.swapaxes(weights, 3, 4))
        return jnp.transpose(got, (3, 0, 1, 2))

    return jax.shard_map(
        on_device,
        mesh=mesh,
        in_specs=(P("ta", "gx", None, None, None), P(None, "gx", None, None, None)),
        out_specs=P(None, None, "gx", "ta"),
        check_vma=False,
    )
```

```python
import jax
import jax.numpy as jnp
from jax import lax
from jax.experimental import pallas as pl
from jax.experimental.pallas import tpu as pltpu
from jax.sharding import PartitionSpec as P

MESH = pl.DeviceIdType.MESH
BF = jnp.bfloat16
F32 = jnp.float32
NX, NY, NZ, NC = 4, 4, 8, 2


def iota(shape, dim):
    return lax.broadcasted_iota(jnp.int32, shape, dim)


def one_hot(cond):
    return jnp.where(cond, 1.0, 0.0).astype(BF)


def dot(a, b):
    return jnp.dot(a, b, preferred_element_type=F32)


def tn_dot(a, b):
    return lax.dot_general(a, b, (((0,), (0,)), ((), ())), preferred_element_type=F32)


def exchange_kernel(x_hbm, w_hbm, out_ref, xv, wv, snd, rcv, amat, acc, snd2, rcv2,
                    line_sem, in_sem, send_sem, recv_sem, send2_sem, recv2_sem):
    ta = lax.axis_index("ta")
    g = lax.axis_index("gx")
    core = lax.rem(g, 2)
    y = lax.rem(lax.div(g, 2), NY)
    z = lax.rem(lax.div(g, 8), NZ)
    x_lo = lax.div(g, 64)
    x = ta * 2 + x_lo
    me = ta * 128 + g
    copy_x = pltpu.make_async_copy(x_hbm, xv, in_sem.at[0])
    copy_w = pltpu.make_async_copy(w_hbm, wv, in_sem.at[1])
    copy_x.start()
    copy_w.start()

    nxs = [lax.rem(x + d, NX) for d in range(NX)]
    tas = [lax.div(v, 2) for v in nxs]
    xbs = [lax.rem(v, 2) * 64 for v in nxs]
    ybs = [lax.rem(y + d, NY) * 2 for d in range(NY)]
    zbs = [lax.rem(z + d, NZ) * 8 for d in range(NZ)]
    cores = [core, 1 - core]
    far_z = (4, 3, 5, 2, 6, 1, 7, 0)

    def signal(sem, nta, ng):
        pl.semaphore_signal(sem, inc=1, device_id={"ta": nta, "gx": ng}, device_id_type=MESH)

    barrier = pltpu.get_barrier_semaphore()
    corner = x_lo * 64 + y * 2
    line = [corner + zbs[dz] + cores[dc] for dz in far_z for dc in (1, 0)]
    others = [(dx, dy) for dx in (2, 1, 3, 0) for dy in (2, 1, 3, 0)][:-1]
    for ng in line[:-1]:
        signal(barrier, ta, ng)
    for dx, dy in others:
        signal(barrier, tas[dx], xbs[dx] + ybs[dy] + zbs[0] + core)

    r_i, r_k = iota((64, 128), 0), iota((64, 128), 1)
    picked = (r_i & 1) * 64 + (r_i >> 1) * 2
    p_i, p_k = iota((256, 256), 0), iota((256, 256), 1)
    lanes = one_hot(p_i == (p_k & 31) * 8 + (p_k >> 5))
    snd_rows = snd.reshape(1024, 256)

    def prepare(j):
        rows = one_hot(r_k == picked + j)
        grouped = []
        for blk in range(4):
            block = jnp.concatenate([xv[0, blk * 64:(blk + 1) * 64], xv[1, blk * 64:(blk + 1) * 64]], 0)
            grouped.append(dot(rows, block).astype(BF))
        grouped = jnp.concatenate(grouped, 0)
        for h in range(2):
            snd_rows[j * 512 + h * 256:j * 512 + h * 256 + 256, :] = dot(
                grouped[:, h * 256:(h + 1) * 256], lanes).astype(BF)

    copy_x.wait()
    prepare(0)
    prepare(1)
    pl.semaphore_wait(barrier, 30)
    for dx, dy in others:
        signal(line_sem.at[x * 4 + y], tas[dx], xbs[dx] + ybs[dy] + zbs[0] + core)

    def send(j, nta, ng):
        pltpu.make_async_remote_copy(
            snd.at[j * 256 + nta * 128 + ng], rcv.at[j * 256 + me], send_sem.at[j], recv_sem.at[j * 2 + ta],
            device_id={"ta": nta, "gx": ng}, device_id_type=MESH).start()

    def send_own(j):
        for ng in line[:-1]:
            send(j, ta, ng)
        rcv[j * 256 + me] = snd[j * 256 + me]

    def send_line(j, wait):
        def step(i, carry):
            nx = lax.div(i, 8) * 2 + lax.rem(x + i, 2)
            ny = lax.rem(y + 4 - lax.div(lax.rem(i, 8), 2), NY)

            @pl.when((nx != x) | (ny != y))
            def _():
                if wait:
                    pl.semaphore_wait(line_sem.at[nx * 4 + ny], 1)
                nta = lax.div(nx, 2)
                base = lax.rem(nx, 2) * 64 + ny * 2
                for dz in far_z:
                    for dc in (1, 0):
                        send(j, nta, base + zbs[dz] + cores[dc])
            return carry
        return step

    send_own(0)
    lax.fori_loop(0, 16, send_line(0, True), 0)
    send_own(1)
    lax.fori_loop(0, 16, send_line(1, False), 0)

    copy_w.wait()
    b_i, b_k = iota((512, 512), 0), iota((512, 512), 1)
    beams = one_hot(b_i == (b_k & 255) * 2 + (b_k >> 8))
    e_i, e_k = iota((128, 256), 0), iota((128, 256), 1)
    e_ri, e_a = e_i >> 6, e_i & 63
    k_c, k_a, k_ri = e_k >> 7, (e_k >> 1) & 63, e_k & 1
    sign = jnp.where((k_c == 0) & (k_ri == 1), -1.0, 1.0)
    spread = jnp.where((e_a == k_a) & (e_ri == (k_c ^ k_ri)), sign, 0.0).astype(BF)
    for j in range(2):
        for q in range(2):
            both = dot(wv[q, j].reshape(128, 512), beams).astype(BF)
            made = tn_dot(both, spread).astype(BF)
            amat[j * 2 + q, 0:512, :] = made[:, 0:128]
            amat[j * 2 + q, 512:1024, :] = made[:, 128:256]

    rcv_rows = rcv.reshape(1024, 256)
    lane = iota((256, 128), 1)
    low, even = lane < 64, (lane & 32) == 0

    def send2(j, ng):
        pltpu.make_async_remote_copy(
            snd2.at[j * 128 + ng], rcv2.at[j * 128 + g], send2_sem.at[j], recv2_sem.at[j],
            device_id={"ta": ta, "gx": ng}, device_id_type=MESH).start()

    half_plane = [lax.rem(x_lo + dx, 2) * 64 + ybs[dy] + cores[dc]
                  for dx in (1, 0) for dy in (2, 1, 3, 0) for dc in (1, 0)]

    for j in range(2):
        for step in range(2):
            h = ta if step == 0 else 1 - ta
            n = 127 + step
            pltpu.make_async_copy(snd.at[pl.ds(0, n)], rcv.at[pl.ds(0, n)], recv_sem.at[j * 2 + h]).wait()
            for q in range(2):
                start = pl.multiple_of(j * 512 + h * 256 + q * 128, 128)
                field = dot(amat[j * 2 + q], rcv_rows[pl.ds(start, 128), :])
                re, im = field[0:512], field[512:1024]
                power = re * re + im * im
                part = power[:, 0:128] + power[:, 128:256]
                acc[q] = part if step == 0 else acc[q] + part

        fold = []
        for q in range(2):
            a, b = acc[q, 0:256], acc[q, 256:512]
            fold.append(jnp.where(low, a, b) + pltpu.roll(jnp.where(low, b, a), 64, 1))
        other = jnp.where(even, fold[1], fold[0])
        summed = jnp.where(even, fold[0], fold[1]) + jnp.where(
            even, pltpu.roll(other, 96, 1), pltpu.roll(other, 32, 1))
        snd2.reshape(512, 128)[j * 256:(j + 1) * 256, :] = summed

        def send2_step(i, carry):
            far = 4 + (2 * lax.rem(i, 2) - 1) * lax.div(i, 2)
            zz = lax.rem(z + far, NZ)
            for base in half_plane:
                send2(j, base + zz * 8)
            return carry

        lax.fori_loop(1, NZ, send2_step, 0)
        for base in half_plane[:-1]:
            send2(j, base + z * 8)
        rcv2[j * 128 + g] = snd2[j * 128 + g]

    wide = iota((32, 128), 1)
    odd = (wide & 1) == 1

    def place(j):
        for high in range(2):
            turned = rcv2[j * 128:(j + 1) * 128, high, :].T
            for parity in range(2):
                for q in range(2):
                    at = parity * 64 + q * 32
                    for part in range(2):
                        cols = slice(part * 128, (part + 1) * 128)
                        own = jnp.take_along_axis(turned[at:at + 32], (wide >> 1) + part * 64, axis=1)
                        if j == 0:
                            out_ref[q, high * 2 + parity, :, cols] = own
                        else:
                            out_ref[q, high * 2 + parity, :, cols] = jnp.where(
                                odd, own, out_ref[q, high * 2 + parity, :, cols])

    for j in range(2):
        pltpu.make_async_copy(snd2.at[pl.ds(0, 127)], rcv2.at[pl.ds(0, 127)], recv2_sem.at[j]).wait()
        place(j)
    for j in range(2):
        pltpu.make_async_copy(snd.at[pl.ds(0, 255)], rcv.at[pl.ds(0, 255)], send_sem.at[j]).wait()
        pltpu.make_async_copy(snd2.at[pl.ds(0, 127)], rcv2.at[pl.ds(0, 127)], send2_sem.at[j]).wait()


def solution(mesh):
    def on_device(voltages, weights):
        vmem = pl.BlockSpec(memory_space=pltpu.VMEM)
        hbm = pl.BlockSpec(memory_space=pl.ANY)
        got = pl.pallas_call(
            exchange_kernel,
            out_shape=pltpu.VMEM((2, 4, 32, 256), F32),
            in_specs=[hbm, hbm],
            out_specs=vmem,
            scratch_shapes=[
                pltpu.VMEM((2, 256, 512), BF),
                pltpu.VMEM((2, 2, 2, 64, 512), BF),
                pltpu.VMEM((512, 2, 256), BF),
                pltpu.VMEM((512, 2, 256), BF),
                pltpu.VMEM((4, 1024, 128), BF),
                pltpu.VMEM((2, 512, 128), F32),
                pltpu.VMEM((256, 2, 128), F32),
                pltpu.VMEM((256, 2, 128), F32),
                pltpu.SemaphoreType.REGULAR((16,)),
                pltpu.SemaphoreType.DMA((2,)),
                pltpu.SemaphoreType.DMA((2,)),
                pltpu.SemaphoreType.DMA((4,)),
                pltpu.SemaphoreType.DMA((2,)),
                pltpu.SemaphoreType.DMA((2,)),
            ],
            compiler_params=pltpu.CompilerParams(collective_id=0, has_side_effects=True),
        )(voltages[0, 0], jnp.swapaxes(weights, 3, 4))
        return jnp.transpose(got, (3, 0, 1, 2))

    return jax.shard_map(
        on_device,
        mesh=mesh,
        in_specs=(P("ta", "gx", None, None, None), P(None, "gx", None, None, None)),
        out_specs=P(None, None, "gx", "ta"),
        check_vma=False,
    )
```

```python
import jax
import jax.numpy as jnp
from jax import lax
from jax.experimental import pallas as pl
from jax.experimental.pallas import tpu as pltpu
from jax.sharding import PartitionSpec as P

MESH = pl.DeviceIdType.MESH
BF = jnp.bfloat16
F32 = jnp.float32
NX, NY, NZ, NC = 4, 4, 8, 2


def iota(shape, dim):
    return lax.broadcasted_iota(jnp.int32, shape, dim)


def one_hot(cond):
    return jnp.where(cond, 1.0, 0.0).astype(BF)


def dot(a, b):
    return jnp.dot(a, b, preferred_element_type=F32)


def tn_dot(a, b):
    return lax.dot_general(a, b, (((0,), (0,)), ((), ())), preferred_element_type=F32)


def exchange_kernel(x_hbm, w_hbm, out_ref, xv, wv, snd, rcv, amat, acc, snd2, rcv2,
                    line_sem, in_sem, send_sem, recv_sem, send2_sem, recv2_sem):
    ta = lax.axis_index("ta")
    g = lax.axis_index("gx")
    core = lax.rem(g, 2)
    y = lax.rem(lax.div(g, 2), NY)
    z = lax.rem(lax.div(g, 8), NZ)
    x_lo = lax.div(g, 64)
    x = ta * 2 + x_lo
    me = ta * 128 + g
    copy_x = pltpu.make_async_copy(x_hbm, xv, in_sem.at[0])
    copy_w = pltpu.make_async_copy(w_hbm, wv, in_sem.at[1])
    copy_x.start()
    copy_w.start()

    nxs = [lax.rem(x + d, NX) for d in range(NX)]
    tas = [lax.div(v, 2) for v in nxs]
    xbs = [lax.rem(v, 2) * 64 for v in nxs]
    ybs = [lax.rem(y + d, NY) * 2 for d in range(NY)]
    zbs = [lax.rem(z + d, NZ) * 8 for d in range(NZ)]
    cores = [core, 1 - core]
    far_z = (4, 3, 5, 2, 6, 1, 7, 0)

    def signal(sem, nta, ng):
        pl.semaphore_signal(sem, inc=1, device_id={"ta": nta, "gx": ng}, device_id_type=MESH)

    barrier = pltpu.get_barrier_semaphore()
    corner = x_lo * 64 + y * 2
    line = [corner + zbs[dz] + cores[dc] for dz in far_z for dc in (1, 0)]
    others = [(dx, dy) for dx in (2, 1, 3, 0) for dy in (2, 1, 3, 0)][:-1]
    for ng in line[:-1]:
        signal(barrier, ta, ng)
    for dx, dy in others:
        signal(barrier, tas[dx], xbs[dx] + ybs[dy] + zbs[0] + core)

    r_i, r_k = iota((64, 128), 0), iota((64, 128), 1)
    picked = (r_i & 1) * 64 + (r_i >> 1) * 2
    p_i, p_k = iota((256, 256), 0), iota((256, 256), 1)
    lanes = one_hot(p_i == (p_k & 31) * 8 + (p_k >> 5))
    snd_rows = snd.reshape(1024, 256)

    def prepare(j):
        rows = one_hot(r_k == picked + j)
        grouped = []
        for blk in range(4):
            block = jnp.concatenate([xv[0, blk * 64:(blk + 1) * 64], xv[1, blk * 64:(blk + 1) * 64]], 0)
            grouped.append(dot(rows, block).astype(BF))
        grouped = jnp.concatenate(grouped, 0)
        for h in range(2):
            snd_rows[j * 512 + h * 256:j * 512 + h * 256 + 256, :] = dot(
                grouped[:, h * 256:(h + 1) * 256], lanes).astype(BF)

    copy_x.wait()
    prepare(0)
    prepare(1)
    pl.semaphore_wait(barrier, 30)
    for dx, dy in others:
        signal(line_sem.at[x * 4 + y], tas[dx], xbs[dx] + ybs[dy] + zbs[0] + core)

    def send(j, nta, ng):
        pltpu.make_async_remote_copy(
            snd.at[j * 256 + nta * 128 + ng], rcv.at[j * 256 + me], send_sem.at[j], recv_sem.at[j * 2 + ta],
            device_id={"ta": nta, "gx": ng}, device_id_type=MESH).start()

    def send_own(j):
        for ng in line[:-1]:
            send(j, ta, ng)
        rcv[j * 256 + me] = snd[j * 256 + me]

    def send_line(j, wait):
        def step(i, carry):
            nx = lax.div(i, 8) * 2 + lax.rem(x + i, 2)
            ny = lax.rem(y + (1 if wait else 3) * lax.div(lax.rem(i, 8), 2), NY)

            @pl.when((nx != x) | (ny != y))
            def _():
                if wait:
                    pl.semaphore_wait(line_sem.at[nx * 4 + ny], 1)
                nta = lax.div(nx, 2)
                base = lax.rem(nx, 2) * 64 + ny * 2
                for dz in far_z:
                    for dc in (1, 0):
                        send(j, nta, base + zbs[dz] + cores[dc])
            return carry
        return step

    send_own(0)
    lax.fori_loop(0, 16, send_line(0, True), 0)
    send_own(1)
    lax.fori_loop(0, 16, send_line(1, False), 0)

    copy_w.wait()
    b_i, b_k = iota((512, 512), 0), iota((512, 512), 1)
    beams = one_hot(b_i == (b_k & 255) * 2 + (b_k >> 8))
    e_i, e_k = iota((128, 256), 0), iota((128, 256), 1)
    e_ri, e_a = e_i >> 6, e_i & 63
    k_c, k_a, k_ri = e_k >> 7, (e_k >> 1) & 63, e_k & 1
    sign = jnp.where((k_c == 0) & (k_ri == 1), -1.0, 1.0)
    spread = jnp.where((e_a == k_a) & (e_ri == (k_c ^ k_ri)), sign, 0.0).astype(BF)
    for j in range(2):
        for q in range(2):
            both = dot(wv[q, j].reshape(128, 512), beams).astype(BF)
            made = tn_dot(both, spread).astype(BF)
            amat[j * 2 + q, 0:512, :] = made[:, 0:128]
            amat[j * 2 + q, 512:1024, :] = made[:, 128:256]

    rcv_rows = rcv.reshape(1024, 256)
    lane = iota((256, 128), 1)
    low, even = lane < 64, (lane & 32) == 0

    def send2(j, ng):
        pltpu.make_async_remote_copy(
            snd2.at[j * 128 + ng], rcv2.at[j * 128 + g], send2_sem.at[j], recv2_sem.at[j],
            device_id={"ta": ta, "gx": ng}, device_id_type=MESH).start()

    half_plane = [lax.rem(x_lo + dx, 2) * 64 + ybs[dy] + cores[dc]
                  for dx in (1, 0) for dy in (2, 1, 3, 0) for dc in (1, 0)]

    for j in range(2):
        for step in range(2):
            h = ta if step == 0 else 1 - ta
            n = 127 + step
            pltpu.make_async_copy(snd.at[pl.ds(0, n)], rcv.at[pl.ds(0, n)], recv_sem.at[j * 2 + h]).wait()
            for q in range(2):
                start = pl.multiple_of(j * 512 + h * 256 + q * 128, 128)
                field = dot(amat[j * 2 + q], rcv_rows[pl.ds(start, 128), :])
                re, im = field[0:512], field[512:1024]
                power = re * re + im * im
                part = power[:, 0:128] + power[:, 128:256]
                acc[q] = part if step == 0 else acc[q] + part

        fold = []
        for q in range(2):
            a, b = acc[q, 0:256], acc[q, 256:512]
            fold.append(jnp.where(low, a, b) + pltpu.roll(jnp.where(low, b, a), 64, 1))
        other = jnp.where(even, fold[1], fold[0])
        summed = jnp.where(even, fold[0], fold[1]) + jnp.where(
            even, pltpu.roll(other, 96, 1), pltpu.roll(other, 32, 1))
        snd2.reshape(512, 128)[j * 256:(j + 1) * 256, :] = summed

        def send2_step(i, carry):
            far = 4 + (2 * lax.rem(i, 2) - 1) * lax.div(i, 2)
            zz = lax.rem(z + far, NZ)
            for base in half_plane:
                send2(j, base + zz * 8)
            return carry

        lax.fori_loop(1, NZ, send2_step, 0)
        for base in half_plane[:-1]:
            send2(j, base + z * 8)
        rcv2[j * 128 + g] = snd2[j * 128 + g]

    wide = iota((32, 128), 1)
    odd = (wide & 1) == 1

    def place(j):
        for high in range(2):
            turned = rcv2[j * 128:(j + 1) * 128, high, :].T
            for parity in range(2):
                for q in range(2):
                    at = parity * 64 + q * 32
                    for part in range(2):
                        cols = slice(part * 128, (part + 1) * 128)
                        own = jnp.take_along_axis(turned[at:at + 32], (wide >> 1) + part * 64, axis=1)
                        if j == 0:
                            out_ref[q, high * 2 + parity, :, cols] = own
                        else:
                            out_ref[q, high * 2 + parity, :, cols] = jnp.where(
                                odd, own, out_ref[q, high * 2 + parity, :, cols])

    for j in range(2):
        pltpu.make_async_copy(snd2.at[pl.ds(0, 127)], rcv2.at[pl.ds(0, 127)], recv2_sem.at[j]).wait()
        place(j)
    for j in range(2):
        pltpu.make_async_copy(snd.at[pl.ds(0, 255)], rcv.at[pl.ds(0, 255)], send_sem.at[j]).wait()
        pltpu.make_async_copy(snd2.at[pl.ds(0, 127)], rcv2.at[pl.ds(0, 127)], send2_sem.at[j]).wait()


def solution(mesh):
    def on_device(voltages, weights):
        vmem = pl.BlockSpec(memory_space=pltpu.VMEM)
        hbm = pl.BlockSpec(memory_space=pl.ANY)
        got = pl.pallas_call(
            exchange_kernel,
            out_shape=pltpu.VMEM((2, 4, 32, 256), F32),
            in_specs=[hbm, hbm],
            out_specs=vmem,
            scratch_shapes=[
                pltpu.VMEM((2, 256, 512), BF),
                pltpu.VMEM((2, 2, 2, 64, 512), BF),
                pltpu.VMEM((512, 2, 256), BF),
                pltpu.VMEM((512, 2, 256), BF),
                pltpu.VMEM((4, 1024, 128), BF),
                pltpu.VMEM((2, 512, 128), F32),
                pltpu.VMEM((256, 2, 128), F32),
                pltpu.VMEM((256, 2, 128), F32),
                pltpu.SemaphoreType.REGULAR((16,)),
                pltpu.SemaphoreType.DMA((2,)),
                pltpu.SemaphoreType.DMA((2,)),
                pltpu.SemaphoreType.DMA((4,)),
                pltpu.SemaphoreType.DMA((2,)),
                pltpu.SemaphoreType.DMA((2,)),
            ],
            compiler_params=pltpu.CompilerParams(collective_id=0, has_side_effects=True),
        )(voltages[0, 0], jnp.swapaxes(weights, 3, 4))
        return jnp.transpose(got, (3, 0, 1, 2))

    return jax.shard_map(
        on_device,
        mesh=mesh,
        in_specs=(P("ta", "gx", None, None, None), P(None, "gx", None, None, None)),
        out_specs=P(None, None, "gx", "ta"),
        check_vma=False,
    )
```
